32 devices in a mesh: dp: 8 (over z, core), tensor: 4 (over y, x).
Axes of the slice: x: 2, y: 2, z: 4, core: 2. Of those that a mesh axis runs over, the one named last changes fastest.
Arguments:
- queries: bfloat16 [3584, 8192], P('dp', 'tensor'), may hold values from -6 to 6
- features: bfloat16 [16, 384, 8192], P('dp', None, 'tensor'), may hold values from -6 to 6
- kv_weight: bfloat16 [8192, 2048], P('tensor'), may hold values from -0.0625 to 0.0625
- q_gain: float32 [128], replicated, may hold values from 0.5 to 2
- k_gain: float32 [128], replicated, may hold values from 0.5 to 2
- counts: int32 [16], replicated, may hold values from 1 to 16, as said below
- owner: int32 [16], replicated, may hold values from 0 to 15, as said below
Outputs:
- attended: bfloat16 [3584, 8192], P('dp', 'tensor')
The draws below stay inside these ranges and needn't reach their ends.
Inputs may be any that keep to these rules, and one draw needn't show every extreme that they name: `counts`: every sample has 1 to 16 images; in every draw some sample has 16 and some has one. `owner`: there are 2 different shifts c_j, each from 0 to the number of dp indices minus 1; sample s = e * 2 + j goes to slot ((e + c_j) modulo the number of dp indices) * 2 + j, with the same c_j for every e.
All inputs are finite; a program needn't handle non-finite values.
Results may differ from the reference program's by a relative error of at most 0.028.
Values may be sent and summed in bfloat16 or wider, within the bound.
A program may use at most 64 MiB of HBM per device.

```python
import math
import jax
import jax.numpy as jnp
from jax import lax

VIS = 8192
QH = 64
KVH = 8
HD = 128
TXT = 224
PATCH = 24
MAX_IMAGES = 16
SAMP_DEV = 2
SAMPLES = 16
N_TENSOR = 4


def draw_counts(key, part):
    first_key, second_key = jax.random.split(jax.random.fold_in(key, 11), 2)
    drawn = jax.random.randint(first_key, (SAMPLES,), 1, MAX_IMAGES + 1).astype(jnp.int32)
    chosen = jax.random.permutation(second_key, SAMPLES)[:2]
    drawn = drawn.at[chosen[0]].set(MAX_IMAGES)
    drawn = drawn.at[chosen[1]].set(1)
    return drawn.astype(jnp.int32)


def draw_owner(key, part):
    shard_total = SAMPLES // SAMP_DEV
    base_key = jax.random.fold_in(key, 23)
    shift_list = jax.random.permutation(base_key, shard_total).astype(jnp.int32)[:SAMP_DEV]
    encoder = jnp.arange(shard_total, dtype=jnp.int32)[:, None]
    position = jnp.arange(SAMP_DEV, dtype=jnp.int32)[None, :]
    target = (encoder + shift_list[None, :]) % shard_total
    return (target * SAMP_DEV + position).reshape(-1).astype(jnp.int32)


def shard_levels(own_key, extent, cuts, low, largest):
    factor_of = 1.0
    for dim, blocks in cuts:
        draws = jax.random.uniform(jax.random.fold_in(jax.random.fold_in(own_key, 6), dim), (blocks,), jnp.float32, low / len(cuts), largest / len(cuts))
        factor_of = factor_of * jnp.repeat(jnp.exp(draws), extent[dim] // blocks).reshape((-1,) + (1,) * (len(extent) - 1 - dim))
    return factor_of


def scatter_about(own_key, dims, deviation, most, shards=(), kind=jnp.bfloat16):
    result = deviation * jax.random.normal(own_key, dims, jnp.float32)
    if shards:
        result = result * shard_levels(own_key, dims, shards, -0.22, 0.18)
    return jnp.clip(result, -most, most).astype(kind)


def setup_inputs(seed: int = 0) -> dict:
    arg_keys = jax.random.split(jax.random.key(seed), 8)
    queries = scatter_about(arg_keys[0], (SAMPLES * TXT, QH * HD), 1.0, 6.0, ((0, 8), (1, 4)))
    features = scatter_about(arg_keys[1], (SAMPLES, MAX_IMAGES * PATCH, VIS), 1.0, 6.0, ((0, 8), (2, 4)))
    kv_weight = scatter_about(arg_keys[2], (VIS, 2 * KVH * HD), VIS ** -0.5, 0.0625, ((0, 4),))
    q_gain = jnp.clip(jnp.exp(jax.random.uniform(arg_keys[3], (HD,), jnp.float32, math.log(0.5), math.log(2.0))), 0.5, 2.0)
    k_gain = jnp.clip(jnp.exp(jax.random.uniform(arg_keys[4], (HD,), jnp.float32, math.log(0.5), math.log(2.0))), 0.5, 2.0)
    counts = draw_counts(jax.random.fold_in(arg_keys[7], 71), 0)
    owner = draw_owner(jax.random.fold_in(arg_keys[7], 71), 0)
    return {"queries": queries, "features": features, "kv_weight": kv_weight, "q_gain": q_gain, "k_gain": k_gain, "counts": counts, "owner": owner}


def normalize_rows(values_in, gain):
    return values_in * lax.rsqrt(lax.optimization_barrier(jnp.mean(values_in * values_in, axis=-1, keepdims=True)) + 1e-05) * gain

def reference(queries, features, kv_weight, q_gain, k_gain, counts, owner):
    group_size = QH // KVH
    token_count = features.shape[1]
    piece_width = VIS // N_TENSOR
    weight_groups = kv_weight.astype(jnp.float32).reshape(N_TENSOR, piece_width, 2 * KVH * HD)
    source_of = jnp.zeros((SAMPLES,), jnp.int32).at[owner].set(jnp.arange(SAMPLES, dtype=jnp.int32))
    query_blocks = queries.reshape(SAMPLES, TXT, QH, HD)

    def attend_slot(slot_id):
        sample = source_of[slot_id]
        feature_rows = features[sample].astype(jnp.float32).reshape(token_count, N_TENSOR, piece_width)
        partials = jnp.einsum('rnc,ncf->nrf', feature_rows, weight_groups)
        partials = lax.optimization_barrier(partials.astype(jnp.bfloat16)).astype(jnp.float32)
        projected = lax.optimization_barrier(jnp.sum(partials, axis=0)).reshape(token_count, KVH, 2, HD)
        key_heads = normalize_rows(projected[:, :, 0], k_gain).astype(jnp.bfloat16)
        value_heads = projected[:, :, 1].astype(jnp.bfloat16)
        query_here = normalize_rows(query_blocks[slot_id].astype(jnp.float32), q_gain) / math.sqrt(HD)
        query_here = lax.optimization_barrier(query_here.astype(jnp.bfloat16)).astype(jnp.float32)
        key_here = jnp.repeat(key_heads, group_size, axis=1).astype(jnp.float32)
        value_here = jnp.repeat(value_heads, group_size, axis=1).astype(jnp.float32)
        scores = jnp.einsum('tqd,rqd->qtr', query_here, key_here)
        valid_keys = jnp.arange(token_count, dtype=jnp.int32) < counts[sample] * PATCH
        exponent = jnp.where(valid_keys[None, None, :], jnp.exp(scores), 0.0)
        weights = (exponent / lax.optimization_barrier(jnp.sum(exponent, axis=-1, keepdims=True))).astype(jnp.bfloat16)
        weights = lax.optimization_barrier(weights).astype(jnp.float32)
        context = jnp.einsum('qtr,rqd->tqd', weights, value_here)
        return context.astype(jnp.bfloat16).reshape(TXT, QH * HD)
    attended = lax.map(attend_slot, jnp.arange(SAMPLES, dtype=jnp.int32))
    return attended.reshape(SAMPLES * TXT, QH * HD)
```

```python
import functools
import math

import jax
import jax.numpy as jnp
from jax import lax
from jax.experimental import pallas as pl
from jax.experimental.pallas import tpu as pltpu
from jax.sharding import PartitionSpec as P

KVH = 8
HD = 128
PATCH = 24
EPS = 1e-05
MESH = pl.DeviceIdType.MESH
VMEM_LIMIT = 60 * 1024 * 1024


def bit_orders(count):
    bits = [1 << b for b in range(count.bit_length() - 1)]
    return bits, bits[::-1]


def send_round(order, d):
    for r, bit in enumerate(order):
        if d & bit:
            return r
    return len(order)


def project_kernel(n, x_hbm, w_hbm, gain_ref, out_ref, xv, wv, part, recv, x_sem, w_sem, send_sem, recv_sem):
    me = lax.axis_index("tensor")
    half = xv.shape[0] // 2
    width = wv.shape[2]
    orders = bit_orders(n)

    def flipped(d):
        result = me
        for bit in orders[0]:
            if d & bit:
                result = result + bit * (1 - 2 * ((me // bit) % 2))
        return result

    pieces = sorted(
        [(send_round(orders[s], d), -d, s) for d in range(n) for s in range(2)]
    )
    pieces = [(r, -d, s) for r, d, s in pieces]

    def x_copy(s):
        rows = pl.ds(s * half, half)
        return pltpu.make_async_copy(x_hbm.at[rows], xv.at[rows], x_sem.at[s])

    def w_copy(d):
        columns = pl.ds(pl.multiple_of(flipped(d) * width, 128), width)
        return pltpu.make_async_copy(w_hbm.at[:, columns], wv.at[d], w_sem.at[d])

    def remote(d, s):
        bit = orders[s][send_round(orders[s], d)]
        return pltpu.make_async_remote_copy(
            src_ref=part.at[d, s],
            dst_ref=recv.at[s, d - 1],
            send_sem=send_sem.at[s, d - 1],
            recv_sem=recv_sem.at[s, d - 1],
            device_id={"tensor": flipped(bit)},
            device_id_type=MESH,
        )

    barrier = pltpu.get_barrier_semaphore()
    for bit in orders[0]:
        pl.semaphore_signal(barrier, inc=1, device_id={"tensor": flipped(bit)}, device_id_type=MESH)
    x_copy(0).start()
    w_order = []
    for _, d, _ in pieces:
        if d not in w_order:
            w_order.append(d)
    w_copy(w_order[0]).start()
    x_copy(1).start()
    for d in w_order[1:]:
        w_copy(d).start()
    pl.semaphore_wait(barrier, len(orders[0]))

    x_ready, w_ready = set(), set()
    for r, d, s in pieces:
        if s not in x_ready:
            x_copy(s).wait()
            x_ready.add(s)
        if d not in w_ready:
            w_copy(d).wait()
            w_ready.add(d)
        part[d, s] = jnp.dot(
            xv[s * half : (s + 1) * half], wv[d], preferred_element_type=jnp.float32
        ).astype(jnp.bfloat16)
        if r == 0:
            remote(d, s).start()

    def total(d, s):
        result = part[d, s].astype(jnp.float32)
        for bit in orders[s][: send_round(orders[s], d)]:
            remote(d | bit, s).wait_recv()
            result = result + recv[s, (d | bit) - 1].astype(jnp.float32)
        return result

    for r, d, s in pieces:
        if 0 < r and d > 0:
            part[d, s] = total(d, s).astype(jnp.bfloat16)
            remote(d, s).start()
    gain = gain_ref[...]
    for s in range(2):
        summed = total(0, s)
        rows = slice(s * half, (s + 1) * half)
        for c in range(0, width, HD):
            block = summed[:, c : c + HD]
            if c // HD % 2 == 0:
                scale = lax.rsqrt(jnp.mean(block * block, axis=-1, keepdims=True) + EPS)
                block = block * scale * gain
            out_ref[rows, c : c + HD] = block.astype(jnp.bfloat16)
    for _, d, s in pieces:
        if d > 0:
            remote(d, s).wait_send()


def project(flat, weight, k_gain, n):
    rows, channels = flat.shape
    width = weight.shape[1] // n
    half = rows // 2
    return pl.pallas_call(
        functools.partial(project_kernel, n),
        out_shape=jax.ShapeDtypeStruct((rows, width), jnp.bfloat16),
        in_specs=[
            pl.BlockSpec(memory_space=pl.ANY),
            pl.BlockSpec(memory_space=pl.ANY),
            pl.BlockSpec(memory_space=pltpu.VMEM),
        ],
        out_specs=pl.BlockSpec(memory_space=pltpu.VMEM),
        scratch_shapes=[
            pltpu.VMEM((rows, channels), jnp.bfloat16),
            pltpu.VMEM((n, channels, width), jnp.bfloat16),
            pltpu.VMEM((n, 2, half, width), jnp.bfloat16),
            pltpu.VMEM((2, n - 1, half, width), jnp.bfloat16),
            pltpu.SemaphoreType.DMA((2,)),
            pltpu.SemaphoreType.DMA((n,)),
            pltpu.SemaphoreType.DMA((2, n - 1)),
            pltpu.SemaphoreType.DMA((2, n - 1)),
        ],
        compiler_params=pltpu.CompilerParams(
            collective_id=0, has_side_effects=True, vmem_limit_bytes=VMEM_LIMIT
        ),
        cost_estimate=pl.CostEstimate(
            flops=2 * rows * channels * weight.shape[1],
            bytes_accessed=2 * (flat.size + weight.size),
            transcendentals=0,
        ),
        name="project",
    )(flat, weight, k_gain)


def attend_kernel(count_ref, q_ref, gain_ref, kv_ref, out_ref):
    sample = pl.program_id(0)
    tokens = kv_ref.shape[1]
    keys = kv_ref[0, :, :HD]
    values = jnp.concatenate(
        [kv_ref[0, :, HD:], jnp.ones((tokens, HD), jnp.bfloat16)], axis=1
    )
    valid = lax.broadcasted_iota(jnp.int32, (1, tokens), 1) < count_ref[sample] * PATCH
    gain = gain_ref[...] * (1.0 / math.sqrt(HD))
    for head in range(q_ref.shape[1] // HD):
        columns = slice(head * HD, (head + 1) * HD)
        query = q_ref[:, columns].astype(jnp.float32)
        scale = lax.rsqrt(jnp.mean(query * query, axis=-1, keepdims=True) + EPS)
        query = (query * scale * gain).astype(jnp.bfloat16)
        scores = lax.dot_general(
            query, keys, (((1,), (1,)), ((), ())), preferred_element_type=jnp.float32
        )
        weights = jnp.where(valid, jnp.exp(scores), 0.0).astype(jnp.bfloat16)
        both = jnp.dot(weights, values, preferred_element_type=jnp.float32)
        out_ref[:, columns] = (both[:, :HD] / both[:, HD:]).astype(jnp.bfloat16)


def attend(slot_count, queries, q_gain, moved):
    samples, tokens, width = moved.shape
    kv_heads = width // (2 * HD)
    text_len = queries.shape[0] // samples
    group = queries.shape[1] // kv_heads
    return pl.pallas_call(
        attend_kernel,
        out_shape=jax.ShapeDtypeStruct(queries.shape, jnp.bfloat16),
        grid=(samples, kv_heads),
        in_specs=[
            pl.BlockSpec(memory_space=pltpu.SMEM),
            pl.BlockSpec((text_len, group), lambda s, h: (s, h)),
            pl.BlockSpec((1, HD), lambda s, h: (0, 0)),
            pl.BlockSpec((1, tokens, 2 * HD), lambda s, h: (s, 0, h)),
        ],
        out_specs=pl.BlockSpec((text_len, group), lambda s, h: (s, h)),
        name="attend",
    )(slot_count, queries, q_gain.reshape(1, HD), moved)


def shift_by(value, count):
    if count == 0:
        return value
    length = lax.axis_size("dp")
    return lax.ppermute(value, "dp", [(i, (i + count) % length) for i in range(length)])


def shards(queries, features, kv_weight, q_gain, k_gain, counts, owner):
    samples_here, token_count, channels = features.shape
    shard_count = lax.axis_size("dp")
    tensor_count = lax.axis_size("tensor")
    my_index = lax.axis_index("dp")
    local_width = kv_weight.shape[1] // tensor_count
    repeats = max(1, 2 * HD // local_width)
    if repeats > 1:
        weight_used = jnp.repeat(kv_weight.reshape(channels, KVH, 2 * HD), repeats, axis=1)
        weight_used = weight_used.reshape(channels, KVH * repeats * 2 * HD)
    else:
        weight_used = kv_weight
    shifts = owner[:samples_here] // samples_here
    source = (my_index - shifts) % shard_count * samples_here + jnp.arange(
        samples_here, dtype=jnp.int32
    )
    matches = jnp.arange(counts.shape[0], dtype=jnp.int32)[None, :] == source[:, None]
    slot_count = jnp.sum(jnp.where(matches, counts[None, :], 0), axis=1)
    ready = project(
        features.reshape(-1, channels), weight_used, k_gain.reshape(1, HD), tensor_count
    ).reshape(samples_here, token_count, -1)
    branches = [functools.partial(shift_by, count=c) for c in range(shard_count)]
    moved = jnp.stack(
        [lax.switch(shifts[j], branches, ready[j]) for j in range(samples_here)]
    )
    return attend(slot_count, queries, q_gain, moved)


def solution(mesh):
    placed = (P("dp", "tensor"), P("dp", None, "tensor"), P("tensor", None), P(), P(), P(), P())
    return jax.shard_map(
        shards, mesh=mesh, in_specs=placed, out_specs=P("dp", "tensor"), check_vma=False
    )
```

```python
import functools
import math

import jax
import jax.numpy as jnp
from jax import lax
from jax.experimental import pallas as pl
from jax.experimental.pallas import tpu as pltpu
from jax.sharding import PartitionSpec as P

KVH = 8
HD = 128
PATCH = 24
EPS = 1e-05
MESH = pl.DeviceIdType.MESH
MOST_VARIANTS = 16
VMEM_LIMIT = 60 * 1024 * 1024


def bit_orders(count):
    bits = [1 << b for b in range(count.bit_length() - 1)]
    return bits, bits[::-1]


def send_round(order, d):
    for r, bit in enumerate(order):
        if d & bit:
            return r
    return len(order)


def project_kernel(n, shift, x_hbm, w_hbm, gain_ref, moved_ref, *rest):
    stay_refs = rest[:-9]
    xv, wv, part, recv, ready, x_sem, w_sem, send_sem, recv_sem = rest[-9:]
    me = lax.axis_index("tensor")
    samples, tokens = xv.shape[0], xv.shape[1]
    half = tokens // 2
    width = wv.shape[2]
    orders = bit_orders(n)
    move_slot = 2 * samples * (n - 1)

    def flipped(d):
        result = me
        for bit in orders[0]:
            if d & bit:
                result = result + bit * (1 - 2 * ((me // bit) % 2))
        return result

    rounds = [[send_round(order, d) for d in range(n)] for order in orders]
    d_order = sorted(range(n), key=lambda d: (min(rounds[0][d], rounds[1][d]), -d))
    place_of = {d: i for i, d in enumerate(d_order)}
    later = sorted(
        [(rounds[s][d], -d, s) for d in range(1, n) for s in range(2) if rounds[s][d] > 0]
    )

    def x_copy(j):
        return pltpu.make_async_copy(x_hbm.at[j], xv.at[j], x_sem.at[j])

    def w_copy(i, first_column):
        columns = pl.ds(pl.multiple_of(first_column, 128), width)
        return pltpu.make_async_copy(w_hbm.at[:, columns], wv.at[i], w_sem.at[i])

    def remote(j, d, s):
        slot = (j * 2 + s) * (n - 1) + d - 1
        return pltpu.make_async_remote_copy(
            src_ref=part.at[j, place_of[d], pl.ds(s * half, half)],
            dst_ref=recv.at[j, s, d - 1],
            send_sem=send_sem.at[slot],
            recv_sem=recv_sem.at[slot],
            device_id={"tensor": flipped(orders[s][rounds[s][d]])},
            device_id_type=MESH,
        )

    def move(s):
        rows = pl.ds(s * half, half)
        if shift == 0:
            return pltpu.make_async_copy(
                ready.at[rows], moved_ref.at[rows], send_sem.at[move_slot + s]
            )
        return pltpu.make_async_remote_copy(
            src_ref=ready.at[rows],
            dst_ref=moved_ref.at[rows],
            send_sem=send_sem.at[move_slot + s],
            recv_sem=recv_sem.at[move_slot + s],
            device_id={"dp": lax.rem(place + shift, shard_count)},
            device_id_type=MESH,
        )

    shard_count = lax.axis_size("dp")
    place = lax.axis_index("dp")
    barrier = pltpu.get_barrier_semaphore()
    greeted = 0
    for bit in orders[0]:
        pl.semaphore_signal(barrier, inc=1, device_id={"tensor": flipped(bit)}, device_id_type=MESH)
        greeted += 1
    if shift:
        for by in (shift, shard_count - shift):
            other = lax.rem(place + by, shard_count)
            pl.semaphore_signal(barrier, inc=1, device_id={"dp": other}, device_id_type=MESH)
            greeted += 1
    x_copy(0).start()
    for i, d in enumerate(d_order):
        w_copy(i, flipped(d) * width).start()
    for j in range(1, samples):
        x_copy(j).start()

    def total(j, d, s):
        result = part[j, place_of[d], s * half : (s + 1) * half].astype(jnp.float32)
        for bit in orders[s][: rounds[s][d]]:
            remote(j, d | bit, s).wait_recv()
            result = result + recv[j, s, (d | bit) - 1].astype(jnp.float32)
        return result

    def send_later(j):
        for _, negative, s in later:
            d = -negative
            part[j, place_of[d], s * half : (s + 1) * half] = total(j, d, s).astype(jnp.bfloat16)
            remote(j, d, s).start()

    def finish(j):
        gain = gain_ref[...]
        target = ready if j == 0 else stay_refs[j - 1]
        for s in range(2):
            summed = total(j, 0, s)
            rows = slice(s * half, (s + 1) * half)
            for c in range(0, width, HD):
                block = summed[:, c : c + HD]
                if c // HD % 2 == 0:
                    scale = lax.rsqrt(jnp.mean(block * block, axis=-1, keepdims=True) + EPS)
                    block = block * scale * gain
                target[rows, c : c + HD] = block.astype(jnp.bfloat16)
            if j == 0:
                move(s).start()

    @pl.loop(0, samples * n)
    def _(step):
        j = step // n
        i = step % n

        @pl.when(i == 0)
        def _():
            x_copy(j).wait()

        @pl.when(j == 0)
        def _():
            w_copy(i, 0).wait()

        part[j, i] = jnp.dot(xv[j], wv[i], preferred_element_type=jnp.float32).astype(
            jnp.bfloat16
        )

        @pl.when(step == 0)
        def _():
            pl.semaphore_wait(barrier, greeted)

        if samples > 1:

            @pl.when((i == 0) & (j > 0))
            def _():
                send_later(j - 1)

        for k, d in enumerate(d_order):
            streams = [s for s in range(2) if rounds[s][d] == 0]
            if streams:

                @pl.when(i == k)
                def _():
                    for s in streams:
                        remote(j, d, s).start()

    for j in range(samples - 1):
        finish(j)
    send_later(samples - 1)
    finish(samples - 1)
    for j in range(samples):
        for d in range(1, n):
            for s in range(2):
                remote(j, d, s).wait_send()
    for s in range(2):
        move(s).wait()


def project(features, weight, k_gain, n, shift, collective_id):
    samples, tokens, channels = features.shape
    width = weight.shape[1] // n
    count = 2 * samples * (n - 1) + 2
    block = jax.ShapeDtypeStruct((tokens, width), jnp.bfloat16)
    return pl.pallas_call(
        functools.partial(project_kernel, n, shift),
        out_shape=[block] * samples,
        in_specs=[
            pl.BlockSpec(memory_space=pl.ANY),
            pl.BlockSpec(memory_space=pl.ANY),
            pl.BlockSpec(memory_space=pltpu.VMEM),
        ],
        out_specs=[pl.BlockSpec(memory_space=pl.ANY)]
        + [pl.BlockSpec(memory_space=pltpu.VMEM)] * (samples - 1),
        scratch_shapes=[
            pltpu.VMEM((samples, tokens, channels), jnp.bfloat16),
            pltpu.VMEM((n, channels, width), jnp.bfloat16),
            pltpu.VMEM((samples, n, tokens, width), jnp.bfloat16),
            pltpu.VMEM((samples, 2, n - 1, tokens // 2, width), jnp.bfloat16),
            pltpu.VMEM((tokens, width), jnp.bfloat16),
            pltpu.SemaphoreType.DMA((samples,)),
            pltpu.SemaphoreType.DMA((n,)),
            pltpu.SemaphoreType.DMA((count,)),
            pltpu.SemaphoreType.DMA((count,)),
        ],
        compiler_params=pltpu.CompilerParams(
            collective_id=collective_id, has_side_effects=True, vmem_limit_bytes=VMEM_LIMIT
        ),
        name="project",
    )(features, weight, k_gain)


def attend_kernel(sample, samples, count_ref, owner_ref, q_ref, gain_ref, kv_ref, *rest):
    out_ref = rest[-1]
    shard_count = lax.axis_size("dp")
    tokens = kv_ref.shape[0]
    source = lax.axis_index("dp") - owner_ref[sample] // samples + shard_count
    count = count_ref[lax.rem(source, shard_count) * samples + sample]
    keys = kv_ref[:, :HD]
    values = jnp.concatenate([kv_ref[:, HD:], jnp.ones((tokens, HD), jnp.bfloat16)], axis=1)
    valid = lax.broadcasted_iota(jnp.int32, (1, tokens), 1) < count * PATCH
    gain = gain_ref[...] * (1.0 / math.sqrt(HD))
    for head in range(q_ref.shape[1] // HD):
        columns = slice(head * HD, (head + 1) * HD)
        query = q_ref[:, columns].astype(jnp.float32)
        scale = lax.rsqrt(jnp.mean(query * query, axis=-1, keepdims=True) + EPS)
        query = (query * scale * gain).astype(jnp.bfloat16)
        scores = lax.dot_general(
            query, keys, (((1,), (1,)), ((), ())), preferred_element_type=jnp.float32
        )
        weights = jnp.where(valid, jnp.exp(scores), 0.0).astype(jnp.bfloat16)
        both = jnp.dot(weights, values, preferred_element_type=jnp.float32)
        out_ref[:, columns] = (both[:, :HD] / both[:, HD:]).astype(jnp.bfloat16)


def attend(sample, samples, counts, owner, queries, q_gain, kv, out):
    tokens, width = kv.shape
    kv_heads = width // (2 * HD)
    text_len = queries.shape[0] // samples
    group = queries.shape[1] // kv_heads
    smem = pl.BlockSpec(memory_space=pltpu.SMEM)
    operands = [counts, owner, queries, q_gain.reshape(1, HD), kv]
    specs = [
        smem,
        smem,
        pl.BlockSpec((text_len, group), lambda h: (sample, h)),
        pl.BlockSpec((1, HD), lambda h: (0, 0)),
        pl.BlockSpec((tokens, 2 * HD), lambda h: (0, h)),
    ]
    aliases = {}
    if out is not None:
        aliases = {len(operands): 0}
        operands.append(out)
        specs.append(pl.BlockSpec(memory_space=pl.ANY))
    products = 2 * text_len * queries.shape[1] * tokens * 2
    return pl.pallas_call(
        functools.partial(attend_kernel, sample, samples),
        out_shape=jax.ShapeDtypeStruct(queries.shape, jnp.bfloat16),
        grid=(kv_heads,),
        in_specs=specs,
        out_specs=pl.BlockSpec((text_len, group), lambda h: (sample, h)),
        input_output_aliases=aliases,
        cost_estimate=pl.CostEstimate(
            flops=products, bytes_accessed=4 * text_len * queries.shape[1], transcendentals=0
        ),
        name="attend",
    )(*operands)


def shift_by(value, count):
    if count == 0:
        return value
    length = lax.axis_size("dp")
    return lax.ppermute(value, "dp", [(i, (i + count) % length) for i in range(length)])


def shards(queries, features, kv_weight, q_gain, k_gain, counts, owner):
    samples_here, token_count, channels = features.shape
    shard_count = lax.axis_size("dp")
    tensor_count = lax.axis_size("tensor")
    local_width = kv_weight.shape[1] // tensor_count
    repeats = max(1, 2 * HD // local_width)
    if repeats > 1:
        weight_used = jnp.repeat(kv_weight.reshape(channels, KVH, 2 * HD), repeats, axis=1)
        weight_used = weight_used.reshape(channels, KVH * repeats * 2 * HD)
    else:
        weight_used = kv_weight
    shifts = owner // samples_here
    gain = k_gain.reshape(1, HD)

    def first_stage(c):
        return lambda: project(features, weight_used, gain, tensor_count, c, c)

    def attend_one(j, kv, out):
        return attend(j, samples_here, counts, owner, queries, q_gain, kv, out)

    def next_stage(j, c):
        return lambda value, kv, out: (shift_by(value, c), attend_one(j - 1, kv, out))

    def shift_switch(j, value):
        moves = [functools.partial(shift_by, count=c) for c in range(shard_count)]
        return lax.switch(shifts[j], moves, value)

    out = None
    if shard_count > MOST_VARIANTS:
        held = first_stage(0)()
        for j in range(samples_here):
            out = attend_one(j, shift_switch(j, held[j]), out)
        return out
    held = lax.switch(shifts[0], [first_stage(c) for c in range(shard_count)])
    moved = held[0]
    for j in range(1, samples_here):
        stages = [next_stage(j, c) for c in range(shard_count)]
        moved, out = lax.switch(shifts[j], stages, held[j], moved, out)
    return attend_one(samples_here - 1, moved, out)


def solution(mesh):
    placed = (P("dp", "tensor"), P("dp", None, "tensor"), P("tensor", None), P(), P(), P(), P())
    return jax.shard_map(
        shards, mesh=mesh, in_specs=placed, out_specs=P("dp", "tensor"), check_vma=False
    )
```

```python
import functools
import math

import jax
import jax.numpy as jnp
from jax import lax
from jax.experimental import pallas as pl
from jax.experimental.pallas import tpu as pltpu
from jax.sharding import PartitionSpec as P

KVH = 8
HD = 128
PATCH = 24
EPS = 1e-05
MESH = pl.DeviceIdType.MESH
MOST_VARIANTS = 16
VMEM_LIMIT = 60 * 1024 * 1024


def bit_orders(count):
    bits = [1 << b for b in range(count.bit_length() - 1)]
    return bits, bits[::-1]


def send_round(order, d):
    for r, bit in enumerate(order):
        if d & bit:
            return r
    return len(order)


def project_kernel(n, shift, x_hbm, w_hbm, gain_ref, moved_ref, *rest):
    stay_refs = rest[:-9]
    xv, wv, part, recv, ready, x_sem, w_sem, send_sem, recv_sem = rest[-9:]
    me = lax.axis_index("tensor")
    samples, tokens = xv.shape[0], xv.shape[1]
    half = tokens // 2
    width = wv.shape[2]
    orders = bit_orders(n)
    move_slot = 2 * samples * (n - 1)

    def flipped(d):
        result = me
        for bit in orders[0]:
            if d & bit:
                result = result + bit * (1 - 2 * ((me // bit) % 2))
        return result

    rounds = [[send_round(order, d) for d in range(n)] for order in orders]
    d_order = sorted(range(n), key=lambda d: (min(rounds[0][d], rounds[1][d]), -d))
    place_of = {d: i for i, d in enumerate(d_order)}
    later = sorted(
        [(rounds[s][d], -d, s) for d in range(1, n) for s in range(2) if rounds[s][d] > 0]
    )

    def x_copy(j):
        return pltpu.make_async_copy(x_hbm.at[j], xv.at[j], x_sem.at[j])

    def w_copy(i, first_column):
        columns = pl.ds(pl.multiple_of(first_column, 128), width)
        return pltpu.make_async_copy(w_hbm.at[:, columns], wv.at[i], w_sem.at[i])

    def remote(j, d, s):
        slot = (j * 2 + s) * (n - 1) + d - 1
        return pltpu.make_async_remote_copy(
            src_ref=part.at[j, place_of[d], pl.ds(s * half, half)],
            dst_ref=recv.at[j, s, d - 1],
            send_sem=send_sem.at[slot],
            recv_sem=recv_sem.at[slot],
            device_id={"tensor": flipped(orders[s][rounds[s][d]])},
            device_id_type=MESH,
        )

    def move(s):
        rows = pl.ds(s * half, half)
        if shift == 0:
            return pltpu.make_async_copy(
                ready.at[rows], moved_ref.at[rows], send_sem.at[move_slot + s]
            )
        return pltpu.make_async_remote_copy(
            src_ref=ready.at[rows],
            dst_ref=moved_ref.at[rows],
            send_sem=send_sem.at[move_slot + s],
            recv_sem=recv_sem.at[move_slot + s],
            device_id={"dp": lax.rem(place + shift, shard_count)},
            device_id_type=MESH,
        )

    shard_count = lax.axis_size("dp")
    place = lax.axis_index("dp")
    barrier = pltpu.get_barrier_semaphore()
    greeted = 0
    for bit in orders[0]:
        pl.semaphore_signal(barrier, inc=1, device_id={"tensor": flipped(bit)}, device_id_type=MESH)
        greeted += 1
    if shift:
        for by in (shift, shard_count - shift):
            other = lax.rem(place + by, shard_count)
            pl.semaphore_signal(barrier, inc=1, device_id={"dp": other}, device_id_type=MESH)
            greeted += 1
    x_copy(0).start()
    for i, d in enumerate(d_order):
        w_copy(i, flipped(d) * width).start()
    for j in range(1, samples):
        x_copy(j).start()

    def total(j, d, s):
        result = part[j, place_of[d], s * half : (s + 1) * half].astype(jnp.float32)
        for bit in orders[s][: rounds[s][d]]:
            remote(j, d | bit, s).wait_recv()
            result = result + recv[j, s, (d | bit) - 1].astype(jnp.float32)
        return result

    def send_later(j):
        for _, negative, s in later:
            d = -negative
            part[j, place_of[d], s * half : (s + 1) * half] = total(j, d, s).astype(jnp.bfloat16)
            remote(j, d, s).start()

    def finish(j):
        gain = gain_ref[...]
        target = ready if j == 0 else stay_refs[j - 1]
        for s in range(2):
            summed = total(j, 0, s)
            rows = slice(s * half, (s + 1) * half)
            for c in range(0, width, HD):
                block = summed[:, c : c + HD]
                if c // HD % 2 == 0:
                    scale = lax.rsqrt(jnp.mean(block * block, axis=-1, keepdims=True) + EPS)
                    block = block * scale * gain
                target[rows, c : c + HD] = block.astype(jnp.bfloat16)
            if j == 0:
                move(s).start()

    @pl.loop(0, samples * n)
    def _(step):
        j = step // n
        i = step % n

        @pl.when(i == 0)
        def _():
            x_copy(j).wait()

        @pl.when(j == 0)
        def _():
            w_copy(i, 0).wait()

        part[j, i] = jnp.dot(xv[j], wv[i], preferred_element_type=jnp.float32).astype(
            jnp.bfloat16
        )

        @pl.when(step == 0)
        def _():
            pl.semaphore_wait(barrier, greeted)

        if samples > 1:

            @pl.when((i == 0) & (j > 0))
            def _():
                send_later(j - 1)

        for k, d in enumerate(d_order):
            streams = [s for s in range(2) if rounds[s][d] == 0]
            if streams:

                @pl.when(i == k)
                def _():
                    for s in streams:
                        remote(j, d, s).start()

    for j in range(samples - 1):
        finish(j)
    send_later(samples - 1)
    finish(samples - 1)
    for j in range(samples):
        for d in range(1, n):
            for s in range(2):
                remote(j, d, s).wait_send()
    for s in range(2):
        move(s).wait()


def project(features, weight, k_gain, n, shift, collective_id):
    samples, tokens, channels = features.shape
    width = weight.shape[1] // n
    count = 2 * samples * (n - 1) + 2
    block = jax.ShapeDtypeStruct((tokens, width), jnp.bfloat16)
    return pl.pallas_call(
        functools.partial(project_kernel, n, shift),
        out_shape=[block] * samples,
        in_specs=[
            pl.BlockSpec(memory_space=pl.ANY),
            pl.BlockSpec(memory_space=pl.ANY),
            pl.BlockSpec(memory_space=pltpu.VMEM),
        ],
        out_specs=[pl.BlockSpec(memory_space=pl.ANY)]
        + [pl.BlockSpec(memory_space=pltpu.VMEM)] * (samples - 1),
        scratch_shapes=[
            pltpu.VMEM((samples, tokens, channels), jnp.bfloat16),
            pltpu.VMEM((n, channels, width), jnp.bfloat16),
            pltpu.VMEM((samples, n, tokens, width), jnp.bfloat16),
            pltpu.VMEM((samples, 2, n - 1, tokens // 2, width), jnp.bfloat16),
            pltpu.VMEM((tokens, width), jnp.bfloat16),
            pltpu.SemaphoreType.DMA((samples,)),
            pltpu.SemaphoreType.DMA((n,)),
            pltpu.SemaphoreType.DMA((count,)),
            pltpu.SemaphoreType.DMA((count,)),
        ],
        compiler_params=pltpu.CompilerParams(
            collective_id=collective_id, has_side_effects=True, vmem_limit_bytes=VMEM_LIMIT
        ),
        name="project",
    )(features, weight, k_gain)


def attend_kernel(sample, samples, count_ref, owner_ref, q_ref, gain_ref, kv_ref, *rest):
    out_ref = rest[-1]
    shard_count = lax.axis_size("dp")
    tokens = kv_ref.shape[0]
    source = lax.axis_index("dp") - lax.div(owner_ref[sample], samples) + shard_count
    count = count_ref[lax.rem(source, shard_count) * samples + sample]
    text_len = q_ref.shape[0]
    keys = kv_ref[:, :HD]
    valid = lax.broadcasted_iota(jnp.int32, (tokens, 1), 0) < count * PATCH
    values = jnp.concatenate([kv_ref[:, HD:], jnp.ones((tokens, HD), jnp.bfloat16)], axis=1)
    values = jnp.where(valid, values.astype(jnp.float32), 0.0).astype(jnp.bfloat16)
    gain = gain_ref[...] * (1.0 / math.sqrt(HD))
    heads = q_ref.shape[1] // HD
    together = 2 if heads % 2 == 0 else 1

    def normed(head):
        query = q_ref[:, head * HD : (head + 1) * HD].astype(jnp.float32)
        scale = lax.rsqrt(jnp.mean(query * query, axis=-1, keepdims=True) + EPS)
        return (query * scale * gain).astype(jnp.bfloat16)

    for first in range(0, heads, together):
        query = jnp.concatenate([normed(first + k) for k in range(together)], axis=0)
        scores = lax.dot_general(
            query, keys, (((1,), (1,)), ((), ())), preferred_element_type=jnp.float32
        )
        weights = jnp.exp(scores).astype(jnp.bfloat16)
        both = jnp.dot(weights, values, preferred_element_type=jnp.float32)
        result = (both[:, :HD] / both[:, HD:]).astype(jnp.bfloat16)
        for k in range(together):
            columns = slice((first + k) * HD, (first + k + 1) * HD)
            out_ref[:, columns] = result[k * text_len : (k + 1) * text_len]


def attend(sample, samples, counts, owner, queries, q_gain, kv, out):
    tokens, width = kv.shape
    kv_heads = width // (2 * HD)
    text_len = queries.shape[0] // samples
    group = queries.shape[1] // kv_heads
    smem = pl.BlockSpec(memory_space=pltpu.SMEM)
    operands = [counts, owner, queries, q_gain.reshape(1, HD), kv]
    specs = [
        smem,
        smem,
        pl.BlockSpec((text_len, group), lambda h: (sample, h)),
        pl.BlockSpec((1, HD), lambda h: (0, 0)),
        pl.BlockSpec((tokens, 2 * HD), lambda h: (0, h)),
    ]
    aliases = {}
    if out is not None:
        aliases = {len(operands): 0}
        operands.append(out)
        specs.append(pl.BlockSpec(memory_space=pl.ANY))
    products = 2 * text_len * queries.shape[1] * tokens * 2
    return pl.pallas_call(
        functools.partial(attend_kernel, sample, samples),
        out_shape=jax.ShapeDtypeStruct(queries.shape, jnp.bfloat16),
        grid=(kv_heads,),
        in_specs=specs,
        out_specs=pl.BlockSpec((text_len, group), lambda h: (sample, h)),
        input_output_aliases=aliases,
        cost_estimate=pl.CostEstimate(
            flops=products, bytes_accessed=4 * text_len * queries.shape[1], transcendentals=0
        ),
        name="attend",
    )(*operands)


def shift_by(value, count):
    if count == 0:
        return value
    length = lax.axis_size("dp")
    return lax.ppermute(value, "dp", [(i, (i + count) % length) for i in range(length)])


def shards(queries, features, kv_weight, q_gain, k_gain, counts, owner):
    samples_here, token_count, channels = features.shape
    shard_count = lax.axis_size("dp")
    tensor_count = lax.axis_size("tensor")
    local_width = kv_weight.shape[1] // tensor_count
    repeats = max(1, 2 * HD // local_width)
    if repeats > 1:
        weight_used = jnp.repeat(kv_weight.reshape(channels, KVH, 2 * HD), repeats, axis=1)
        weight_used = weight_used.reshape(channels, KVH * repeats * 2 * HD)
    else:
        weight_used = kv_weight
    shifts = [lax.div(owner[j], jnp.int32(samples_here)) for j in range(samples_here)]
    gain = k_gain.reshape(1, HD)

    def first_stage(c):
        return lambda: project(features, weight_used, gain, tensor_count, c, c)

    def attend_one(j, kv, out):
        return attend(j, samples_here, counts, owner, queries, q_gain, kv, out)

    def next_stage(j, c):
        return lambda value, kv, out: (shift_by(value, c), attend_one(j - 1, kv, out))

    def shift_switch(j, value):
        moves = [functools.partial(shift_by, count=c) for c in range(shard_count)]
        return lax.switch(shifts[j], moves, value)

    out = None
    if shard_count > MOST_VARIANTS:
        held = first_stage(0)()
        for j in range(samples_here):
            out = attend_one(j, shift_switch(j, held[j]), out)
        return out
    held = lax.switch(shifts[0], [first_stage(c) for c in range(shard_count)])
    moved = held[0]
    for j in range(1, samples_here):
        stages = [next_stage(j, c) for c in range(shard_count)]
        moved, out = lax.switch(shifts[j], stages, held[j], moved, out)
    return attend_one(samples_here - 1, moved, out)


def solution(mesh):
    placed = (P("dp", "tensor"), P("dp", None, "tensor"), P("tensor", None), P(), P(), P(), P())
    return jax.shard_map(
        shards, mesh=mesh, in_specs=placed, out_specs=P("dp", "tensor"), check_vma=False
    )
```
